256 devices in a mesh: expert: 8 (over x, core), dp: 32 (over y, z).
Axes of the slice: x: 4, y: 4, z: 8, core: 2. Of those that a mesh axis runs over, the one named last changes fastest.
Arguments:
- tokens: bfloat16 [32768, 1024], P(('expert', 'dp')), may hold values from -6 to 6
- norm_gain: float32 [1024], replicated, may hold values from 0.1 to 1.9
- router_weight: bfloat16 [1024, 8], replicated, may hold values from -0.3984375 to 0.3984375
- shared_gate_vector: float32 [1024], replicated, may hold values from -0.4 to 0.4
- expert_ids: int32 [32768, 2], P(('expert', 'dp')), may hold values from 0 to 7, all different within a row; in each aligned block of 128 rows (0 to 127, 128 to 255, ...) at most 48 rows name the same one
- gate_weight: bfloat16 [8, 1024, 4096], P('expert', None, 'dp'), may hold values from -0.1875 to 0.1875
- up_weight: bfloat16 [8, 1024, 4096], P('expert', None, 'dp'), may hold values from -0.1875 to 0.1875
- down_weight: bfloat16 [8, 1024, 4096], P('expert', None, 'dp'), may hold values from -0.09375 to 0.09375
- shared_gate_weight: bfloat16 [1024, 4096], P(None, 'expert'), may hold values from -0.1875 to 0.1875
- shared_up_weight: bfloat16 [1024, 4096], P(None, 'expert'), may hold values from -0.1875 to 0.1875
- shared_down_weight: bfloat16 [4096, 1024], P('expert'), may hold values from -0.09375 to 0.09375
Outputs:
- mixed: bfloat16 [32768, 1024], P(('expert', 'dp'))
The draws below stay inside these ranges and needn't reach their ends.
Inputs may be any that keep to these rules, and one draw needn't show every extreme that they name: `expert_ids`: in each aligned block of 128 rows (the rows of one device) no expert is named by more than 48 pairs, and in some block one expert is named by exactly 48; the two ids of a row differ.
All inputs are finite; a program needn't handle non-finite values.
Results may differ from the reference program's by a relative error of at most 0.0085.
Values may be sent and summed in bfloat16 or wider, within the bound.
No kernel may reach another device: no remote copies, remote signals or barrier semaphores. Data moves between devices by JAX's collectives and lax.ppermute only.
A program may use at most 128 MiB of HBM per device.

```python
import math
import jax
import jax.numpy as jnp
import numpy as np
from jax import lax

D = 1024
FF = 4096
SFF = 4096
TOK_DEV = 128
EXPERTS = 8
CAP = 48
TOKENS = 32768
N_EXPERT = 8


def shard_levels(stream_key, extent, shards, least, top_value):
    factor_of = 1.0
    for axis_at, parts in shards:
        steps = jax.random.uniform(jax.random.fold_in(jax.random.fold_in(stream_key, 6), axis_at), (parts,), jnp.float32, least / len(shards), top_value / len(shards))
        factor_of = factor_of * jnp.repeat(jnp.exp(steps), extent[axis_at] // parts).reshape((-1,) + (1,) * (len(extent) - 1 - axis_at))
    return factor_of


def routed_block(rng, own, number, rows, count, top, reach, skew):
    sequence = jax.random.permutation(rng, count)
    heavy_load, common = shares(count, rows * top, reach, skew, True), shares(count, rows * top, reach, skew, False)
    places = jnp.arange(count)

    def named(tallies, rotation):
        used = int((tallies > 0).sum())
        fixed = max(1, used // 4)
        shifted = fixed + (places - fixed + rotation * (used - fixed)) % max(1, count - fixed)
        return jnp.zeros((count,), jnp.int32).at[sequence[jnp.where(places < fixed, places, shifted)]].set(jnp.asarray(tallies, jnp.int32))

    tallies = jnp.where(number % 4 == 0, named(heavy_load, number // 4), named(common, number - number // 4 - 1))
    mixed = jax.random.permutation(jax.random.fold_in(own, 3), count)
    donor, receiver = mixed[0:count // 2 * 2:2], mixed[1:count // 2 * 2:2]
    room = jnp.minimum(tallies[donor] - 1, reach - tallies[receiver]) // 2
    room = jnp.where((donor == sequence[0]) | (receiver == sequence[0]) | (tallies[receiver] == 0), 0, jnp.maximum(room, 0))
    shifted = jax.random.randint(jax.random.fold_in(own, 4), (count // 2,), 0, 1 << 20) % (room + 1)
    tallies = tallies.at[donor].add(-shifted).at[receiver].add(shifted)
    items = jnp.searchsorted(jnp.cumsum(tallies), jnp.arange(rows * top), side="right").astype(jnp.int32)
    listing = items.reshape(top, rows).T
    listing = listing[jax.random.permutation(jax.random.fold_in(own, 1), rows)]
    rotation = jax.random.randint(jax.random.fold_in(own, 2), (rows, 1), 0, top)
    return jnp.take_along_axis(listing, (jnp.arange(top)[None, :] + rotation) % top, axis=1)


def shares(number_of, total, bound, lean, full):
    portions = [(1 << 20) // math.isqrt(rank ** lean) + 1 for rank in range(1, number_of + 1)]
    largest = bound if full else min(bound, max(-(-total // number_of), total * portions[0] // sum(portions)))
    least = 1 if total - largest >= number_of - 1 else 0
    holding, surplus = [largest] + [least] * (number_of - 1), total - largest - least * (number_of - 1)
    while surplus > 0:
        movable = [i for i in range(1, number_of) if holding[i] < largest] or [i for i in range(1, number_of) if holding[i] < bound]
        mass, remaining = sum([portions[i] for i in movable]), surplus
        for i in movable:
            addition = min(bound - holding[i], max(1, remaining * portions[i] // mass), surplus)
            holding[i] = holding[i] + addition
            surplus = surplus - addition
    return np.array(holding)


def bell_draw(own_key, shape, spread, limit, cuts=(), kind=jnp.bfloat16):
    values = spread * jax.random.normal(own_key, shape, jnp.float32)
    if cuts:
        values = values * shard_levels(own_key, shape, cuts, -0.22, 0.18)
    return jnp.clip(values, -limit, limit).astype(kind)


def setup_inputs(seed: int = 0) -> dict:
    arg_keys = jax.random.split(jax.random.key(seed), 12)
    tokens = bell_draw(arg_keys[0], (TOKENS, D), 1.0, 6.0, ((0, 256),))
    norm_gain = jnp.clip(1.0 + 0.18 * jax.random.normal(arg_keys[1], (D,), jnp.float32), 0.1, 1.9)
    router_weight = bell_draw(arg_keys[2], (D, EXPERTS), 0.0625, 0.3984375)
    shared_gate_vector = bell_draw(arg_keys[3], (D,), 0.0625, 0.4, (), jnp.float32)
    expert_ids_keys = jax.random.split(jax.random.fold_in(arg_keys[4], 1), TOKENS // TOK_DEV)
    expert_ids_turns = jax.random.permutation(jax.random.fold_in(arg_keys[4], 3), TOKENS // TOK_DEV)
    expert_ids = jax.vmap(lambda own, number: routed_block(jax.random.fold_in(arg_keys[4], 2), own, number, TOK_DEV, EXPERTS, 2, CAP, 2))(expert_ids_keys, expert_ids_turns).reshape((TOKENS, 2))
    gate_weight = bell_draw(arg_keys[5], (EXPERTS, D, FF), D ** -0.5, 0.1875, ((0, 8), (2, 32)))
    up_weight = bell_draw(arg_keys[6], (EXPERTS, D, FF), D ** -0.5, 0.1875, ((0, 8), (2, 32)))
    down_weight = bell_draw(arg_keys[7], (EXPERTS, D, FF), FF ** -0.5, 0.09375, ((0, 8), (2, 32)))
    shared_gate_weight = bell_draw(arg_keys[8], (D, SFF), D ** -0.5, 0.1875, ((1, 8),))
    shared_up_weight = bell_draw(arg_keys[9], (D, SFF), D ** -0.5, 0.1875, ((1, 8),))
    shared_down_weight = bell_draw(arg_keys[10], (SFF, D), SFF ** -0.5, 0.09375, ((0, 8),))
    return dict(tokens=tokens, norm_gain=norm_gain, router_weight=router_weight, shared_gate_vector=shared_gate_vector, expert_ids=expert_ids, gate_weight=gate_weight, up_weight=up_weight, down_weight=down_weight, shared_gate_weight=shared_gate_weight, shared_up_weight=shared_up_weight, shared_down_weight=shared_down_weight)


def rms_norm(values, gain):
    floats = values.astype(jnp.float32)
    mean_square = lax.optimization_barrier(jnp.mean(floats * floats, axis=-1, keepdims=True))
    return (floats * lax.rsqrt(mean_square + 1e-06) * gain).astype(jnp.bfloat16)

def routing(normed, router_weight, expert_ids):
    logits = jnp.dot(normed, router_weight, preferred_element_type=jnp.float32)
    onehot = expert_ids[:, :, None] == jnp.arange(router_weight.shape[1], dtype=jnp.int32)[None, None, :]
    picked = lax.optimization_barrier(jnp.sum(jnp.where(onehot, logits[:, None, :], jnp.float32(0.0)), axis=-1))
    first_weight = jax.nn.sigmoid(picked[:, 0] - picked[:, 1])
    return jnp.stack([first_weight, 1.0 - first_weight], axis=1)

def slot_of(block_ids):
    flat_ids = block_ids.reshape(-1)
    onehot = (flat_ids[:, None] == jnp.arange(EXPERTS, dtype=jnp.int32)[None, :]).astype(jnp.int32)
    before = jnp.cumsum(onehot, axis=0) - onehot
    return lax.optimization_barrier(jnp.sum(before * onehot, axis=1)).reshape(block_ids.shape).astype(jnp.int32)

def reference(tokens, norm_gain, router_weight, shared_gate_vector, expert_ids, gate_weight, up_weight, down_weight, shared_gate_weight, shared_up_weight, shared_down_weight):
    normed = rms_norm(tokens, norm_gain)
    route_weight = routing(normed, router_weight, expert_ids)
    num_blocks = TOKENS // TOK_DEV
    slot = jax.vmap(slot_of)(expert_ids.reshape(num_blocks, TOK_DEV, 2)).reshape(TOKENS, 2)
    source_block = (jnp.arange(TOKENS, dtype=jnp.int32) // TOK_DEV).astype(jnp.int32)
    position = (source_block[:, None] * CAP + slot).astype(jnp.int32)
    padded_rows = num_blocks * CAP

    def expert_step(running, expert_index):
        slot_index = jnp.where(expert_ids == expert_index, position, padded_rows).astype(jnp.int32)
        buffer = jnp.zeros((padded_rows, D), jnp.bfloat16)
        buffer = buffer.at[slot_index[:, 0]].set(normed, mode='drop')
        buffer = buffer.at[slot_index[:, 1]].set(normed, mode='drop')
        gate_part = jnp.dot(buffer, gate_weight[expert_index], preferred_element_type=jnp.float32)
        up_part = jnp.dot(buffer, up_weight[expert_index], preferred_element_type=jnp.float32)
        hidden = (jax.nn.silu(gate_part) * up_part).astype(jnp.bfloat16)
        expert_out = lax.dot_general(hidden, down_weight[expert_index], (((1,), (1,)), ((), ())), preferred_element_type=jnp.float32).astype(jnp.bfloat16)
        for column in range(2):
            fetched = expert_out[jnp.minimum(slot_index[:, column], padded_rows - 1)].astype(jnp.float32)
            scale = jnp.where(expert_ids[:, column] == expert_index, route_weight[:, column], jnp.float32(0.0))
            running = running + scale[:, None] * fetched
        return (running, None)
    routed, _ = lax.scan(expert_step, jnp.zeros((TOKENS, D), jnp.float32), jnp.arange(EXPERTS, dtype=jnp.int32))
    block_units = SFF // N_EXPERT
    shared = jnp.zeros((TOKENS, D), jnp.float32)
    for block_index in range(N_EXPERT):
        lower = block_index * block_units
        gate_part = jnp.dot(normed, shared_gate_weight[:, lower:lower + block_units], preferred_element_type=jnp.float32)
        up_part = jnp.dot(normed, shared_up_weight[:, lower:lower + block_units], preferred_element_type=jnp.float32)
        hidden = (jax.nn.silu(gate_part) * up_part).astype(jnp.bfloat16)
        partial_out = jnp.dot(hidden, shared_down_weight[lower:lower + block_units, :], preferred_element_type=jnp.float32).astype(jnp.bfloat16)
        partial_out = lax.optimization_barrier(partial_out)
        shared = shared + partial_out.astype(jnp.float32)
    shared_gate = jax.nn.sigmoid(lax.optimization_barrier(jnp.sum(normed.astype(jnp.float32) * shared_gate_vector, axis=-1)))
    return (routed + shared_gate[:, None] * shared).astype(jnp.bfloat16)
```

```python
import functools

import jax
import jax.numpy as jnp
from jax import lax
from jax.experimental import pallas as pl
from jax.experimental.pallas import tpu as pltpu
from jax.sharding import Mesh, PartitionSpec as P


BF = jnp.bfloat16
F32 = jnp.float32
CAP = 48
LANES = 128
NONE = 64.0


def kernel_call(fn, outs, limit_mib, *args, smem=0):
    vm = pl.BlockSpec(memory_space=pltpu.VMEM)
    sm = pl.BlockSpec(memory_space=pltpu.SMEM)
    return pl.pallas_call(
        fn,
        out_shape=outs,
        in_specs=[sm] * smem + [vm] * (len(args) - smem),
        out_specs=jax.tree.map(lambda _: vm, outs),
        compiler_params=pltpu.CompilerParams(vmem_limit_bytes=limit_mib << 20),
    )(*args)


def sds(shape, dtype=BF):
    return jax.ShapeDtypeStruct(shape, dtype)


def shift(a, axis, k):
    n = lax.axis_size(axis)
    return lax.ppermute(a, axis, [(i, (i + k) % n) for i in range(n)])


def swap_core(a):
    return lax.ppermute(a, "c", [(0, 1), (1, 0)])


def ring_gather(a, axis):
    half = a.shape[0] // 2
    f = shift(a, axis, 1)
    b = shift(a, axis, -1)
    return f, b, shift(f[:half], axis, 1), shift(b[half:], axis, -1)


def ring_scatter(own, keep_f, msg_f, keep_b, msg_b, axis):
    half = own.shape[0] // 2
    rf = shift(msg_f, axis, 1)
    rb = shift(msg_b, axis, -1)
    sf = (keep_f.astype(F32) + rf[:half].astype(F32)).astype(BF)
    sb = (keep_b.astype(F32) + rb[half:].astype(F32)).astype(BF)
    qf = shift(sf, axis, 1)
    qb = shift(sb, axis, -1)
    top = own[:half].astype(F32) + rb[:half].astype(F32) + qf.astype(F32)
    bot = own[half:].astype(F32) + rf[half:].astype(F32) + qb.astype(F32)
    return top, bot


def prologue_kernel(tok, gain, router, svec, ids, out):
    x = tok[...].astype(F32)
    ms = jnp.mean(x * x, axis=-1, keepdims=True)
    normed = (x * lax.rsqrt(ms + 1e-06) * gain[...]).astype(BF)
    rows, width = normed.shape
    out[:, :width] = normed
    lane = lax.broadcasted_iota(jnp.int32, (rows, LANES), 1)
    expert = lane & 7
    oh0 = (expert == ids[:, 0:1]).astype(F32)
    oh1 = (expert == ids[:, 1:2]).astype(F32)
    both = oh0 + oh1
    before = (
        lax.broadcasted_iota(jnp.int32, (rows, rows), 1)
        < lax.broadcasted_iota(jnp.int32, (rows, rows), 0)
    ).astype(F32).astype(BF)
    count = jnp.dot(before, both.astype(BF), preferred_element_type=F32)
    slot = jnp.where(both > 0, count, NONE)
    logits = jnp.dot(normed, router[...], preferred_element_type=F32)
    first = (lane < 8).astype(F32)
    l0 = jnp.sum(oh0 * first * logits, axis=-1, keepdims=True)
    l1 = jnp.sum(oh1 * first * logits, axis=-1, keepdims=True)
    w0 = jax.nn.sigmoid(l0 - l1)
    w = oh0 * w0 + oh1 * (1.0 - w0)
    gate = jax.nn.sigmoid(
        jnp.sum(normed.astype(F32) * svec[...], axis=-1, keepdims=True)
    )
    w_hi = w.astype(BF).astype(F32)
    g_hi = gate.astype(BF).astype(F32)
    ext = jnp.where(
        lane < 8,
        slot,
        jnp.where(
            lane < 16,
            w_hi,
            jnp.where(
                lane < 24,
                w - w_hi,
                jnp.where(lane == 24, g_hi, jnp.where(lane == 25, gate - g_hi, 0.0)),
            ),
        ),
    )
    out[:, width:] = ext.astype(BF)


def blocks_of(refs):
    out = []
    for j in range(0, len(refs), 5):
        o, f, b, t, u = refs[j : j + 5]
        out += [(o,), (f,), (b,), (t, u)]
    return out


def load(block, cols):
    parts = [r[:, cols] for r in block]
    return parts[0] if len(parts) == 1 else jnp.concatenate(parts, axis=0)


def dispatch_kernel(me, *refs):
    out = refs[-1]
    width = out.shape[1]
    e = me[0]
    sel = (lax.broadcasted_iota(jnp.int32, (8, LANES), 1) == e).astype(F32).astype(BF)
    s_iota = lax.broadcasted_iota(jnp.int32, (CAP, LANES), 0).astype(F32)
    for j, block in enumerate(blocks_of(refs[:-1])):
        ext = load(block, slice(width, width + LANES))
        slot = lax.dot_general(sel, ext, (((1,), (1,)), ((), ())), preferred_element_type=F32)
        table = (s_iota == slot[0:1, :]).astype(F32).astype(BF)
        x = load(block, slice(0, width))
        out[j * CAP : (j + 1) * CAP, :] = jnp.dot(
            table, x, preferred_element_type=F32
        ).astype(BF)


def shared_kernel(*refs):
    toks, (sg, su, sd, out) = refs[:-4], refs[-4:]
    width = out.shape[1]
    for j, block in enumerate(blocks_of(toks)):
        x = load(block, slice(0, width))
        g = jnp.dot(x, sg[...], preferred_element_type=F32)
        u = jnp.dot(x, su[...], preferred_element_type=F32)
        h = (jax.nn.silu(g) * u).astype(BF)
        n = x.shape[0]
        out[j * n : (j + 1) * n, :] = jnp.dot(
            h, sd[...], preferred_element_type=F32
        ).astype(BF)


def hidden_kernel(n_rows, n_shards, *refs):
    rows = refs[:n_rows]
    wa = refs[n_rows : n_rows + n_shards]
    wb = refs[n_rows + n_shards : n_rows + 2 * n_shards]
    out = refs[-1]
    at = 0
    for r in rows:
        x = r[...]
        n, width = x.shape
        for k in range(n_shards):
            gu = jnp.concatenate([wa[k][:width, :], wb[k][:width, :]], axis=1)
            y = jnp.dot(x, gu, preferred_element_type=F32)
            g, u = y[:, :LANES], y[:, LANES:]
            out[at : at + n, k * LANES : (k + 1) * LANES] = (
                jax.nn.silu(g) * u
            ).astype(BF)
        at += n


def last_hidden_kernel(n_rows, *refs):
    rows = refs[:n_rows]
    a0, a1, b0, b1, out = refs[n_rows:]
    at = 0
    for r in rows:
        x = r[...]
        n, width = x.shape
        lo = a0.shape[0]
        gu = jnp.concatenate(
            [
                jnp.concatenate([a0[...], a1[: width - lo, :]], axis=0),
                jnp.concatenate([b0[...], b1[: width - lo, :]], axis=0),
            ],
            axis=1,
        )
        y = jnp.dot(x, gu, preferred_element_type=F32)
        g, u = y[:, :LANES], y[:, LANES:]
        out[at : at + n, :] = (jax.nn.silu(g) * u).astype(BF)
        at += n


def down_kernel(n_shards, width, h, h_last, *refs):
    shards = refs[:n_shards]
    last = refs[n_shards]
    own, keep_f, msg_f, keep_b, msg_b = refs[n_shards + 1 :]
    d = own.shape[1]
    w = jnp.concatenate(
        [s[width:, :] for s in shards] + [last[last.shape[0] - d :, :]], axis=1
    )
    n = own.shape[0]
    half = n // 2

    def part(lo, size):
        x = jnp.concatenate([h[lo : lo + size, :], h_last[lo : lo + size, :]], axis=1)
        return lax.dot_general(
            x, w, (((1,), (1,)), ((), ())), preferred_element_type=F32
        )

    opp = part(3 * n, n)
    msg_f[:half, :] = opp[:half].astype(BF)
    msg_b[half:, :] = opp[half:].astype(BF)
    nxt = part(2 * n, n)
    keep_f[...] = nxt[:half]
    msg_f[half:, :] = nxt[half:].astype(BF)
    prv = part(n, n)
    msg_b[:half, :] = prv[:half].astype(BF)
    keep_b[...] = prv[half:]
    own[...] = part(0, n)


def combine_kernel(lo, me, top, bot, shared, *refs):
    toks = refs[:10]
    mine, theirs = refs[10:]
    width = shared.shape[1]
    d = top.shape[1]
    e = me[0]
    row = lax.broadcasted_iota(jnp.int32, (LANES, LANES), 0)
    pick_slot = (row == e).astype(F32).astype(BF)
    pick_w = ((row == e + 8) | (row == e + 16)).astype(F32).astype(BF)
    pick_g = ((row == 24) | (row == 25)).astype(F32).astype(BF)
    rows = jnp.concatenate([top[...], bot[...]], axis=0).astype(BF)
    for j, block in enumerate(blocks_of(toks)):
        ext = load(block, slice(width, width + LANES))
        n = ext.shape[0]
        slot = jnp.dot(ext, pick_slot, preferred_element_type=F32)
        w = jnp.dot(ext, pick_w, preferred_element_type=F32)[:, 0:1]
        g = jnp.dot(ext, pick_g, preferred_element_type=F32)[:, 0:1]
        lane = lax.broadcasted_iota(jnp.int32, (n, CAP), 1).astype(F32)
        table = (slot[:, :CAP] == lane).astype(F32).astype(BF)
        got = jnp.dot(
            table, rows[j * CAP : (j + 1) * CAP, :], preferred_element_type=F32
        )
        val = w * got + g * shared[j * n : (j + 1) * n, lo : lo + d].astype(F32)
        if j < 4:
            mine[j * n : (j + 1) * n, :] = val
        else:
            theirs[(j - 4) * n : (j - 3) * n, :] = val.astype(BF)


def body(
    tokens,
    norm_gain,
    router_weight,
    shared_gate_vector,
    expert_ids,
    gate_weight,
    up_weight,
    down_weight,
    shared_gate_weight,
    shared_up_weight,
    shared_down_weight,
):
    n_tok, width = tokens.shape
    half_d = width // 2
    me = (lax.axis_index("x") * 2 + lax.axis_index("c")).astype(jnp.int32)[None]

    wa = jnp.concatenate([gate_weight[0], down_weight[0, :half_d]], axis=0)
    wb = jnp.concatenate([up_weight[0], down_weight[0, half_d:]], axis=0)
    got_a, got_b, last_a, last_b = [wa], [wb], None, None
    fa, ba, fb, bb = wa, wa, wb, wb
    for _ in range(3):
        fa, ba = shift(fa, "z", 1), shift(ba, "z", -1)
        fb, bb = shift(fb, "z", 1), shift(bb, "z", -1)
        got_a += [fa, ba]
        got_b += [fb, bb]
    cut = wa.shape[0] // 2
    last_a = (shift(fa[:cut], "z", 1), shift(ba[cut:], "z", -1))
    last_b = (shift(fb[:cut], "z", 1), shift(bb[cut:], "z", -1))

    router = jnp.concatenate([router_weight] * (LANES // router_weight.shape[1]), axis=1)
    ext = kernel_call(
        prologue_kernel,
        sds((n_tok, width + LANES)),
        16,
        tokens,
        norm_gain[None],
        router,
        shared_gate_vector[None],
        expert_ids,
    )
    f, b, o0, o1 = ring_gather(ext, "x")
    mine = [ext, f, b, o0, o1]
    toks = mine + [swap_core(t) for t in mine]
    rows = kernel_call(
        dispatch_kernel, sds((8 * CAP, width)), 16, me, *toks, smem=1
    )
    rf, rb, ro0, ro1 = ring_gather(rows, "y")
    all_rows = [rows, rf, rb, ro0, ro1]
    shared = kernel_call(
        shared_kernel,
        sds((8 * n_tok, width)),
        24,
        *toks,
        shared_gate_weight,
        shared_up_weight,
        shared_down_weight,
    )
    n_rows = 4 * rows.shape[0]
    n_shards = len(got_a)
    hidden = kernel_call(
        functools.partial(hidden_kernel, len(all_rows), n_shards),
        sds((n_rows, n_shards * LANES)),
        24,
        *all_rows,
        *got_a,
        *got_b,
    )
    hidden_last = kernel_call(
        functools.partial(last_hidden_kernel, len(all_rows)),
        sds((n_rows, LANES)),
        24,
        *all_rows,
        *last_a,
        *last_b,
    )
    n = rows.shape[0]
    outs = []
    for d, (shards, last) in enumerate(((got_a, last_a[1]), (got_b, last_b[1]))):
        parts = kernel_call(
            functools.partial(down_kernel, n_shards, width),
            (
                sds((n, half_d), F32),
                sds((n // 2, half_d), F32),
                sds((n, half_d)),
                sds((n // 2, half_d), F32),
                sds((n, half_d)),
            ),
            24,
            hidden,
            hidden_last,
            *shards,
            last,
        )
        top, bot = ring_scatter(*parts, "y")
        mine_part, theirs = kernel_call(
            functools.partial(combine_kernel, d * half_d),
            (sds((4 * n_tok, half_d), F32), sds((4 * n_tok, half_d))),
            24,
            me,
            top,
            bot,
            shared,
            *toks,
            smem=1,
        )
        s = mine_part + swap_core(theirs).astype(F32)
        own, prv, nxt, opp = (s[i * n_tok : (i + 1) * n_tok] for i in range(4))
        h = n_tok // 2
        msg_f = jnp.concatenate([opp[:h], nxt[h:]], axis=0).astype(BF)
        msg_b = jnp.concatenate([prv[:h], opp[h:]], axis=0).astype(BF)
        top, bot = ring_scatter(own, nxt[:h], msg_f, prv[h:], msg_b, "x")
        outs.append(jnp.concatenate([top, bot], axis=0))
    return jnp.concatenate(outs, axis=1).astype(BF)


def solution(mesh):
    fine = Mesh(mesh.devices.reshape(4, 2, 4, 8), ("x", "c", "y", "z"))
    every = ("x", "c", "y", "z")
    return jax.shard_map(
        body,
        mesh=fine,
        in_specs=(
            P(every, None),
            P(),
            P(),
            P(),
            P(every, None),
            P(("x", "c"), None, ("y", "z")),
            P(("x", "c"), None, ("y", "z")),
            P(("x", "c"), None, ("y", "z")),
            P(None, ("x", "c")),
            P(None, ("x", "c")),
            P(("x", "c"), None),
        ),
        out_specs=P(every, None),
        check_vma=False,
    )
```

```python
import functools

import jax
import jax.numpy as jnp
from jax import lax
from jax.experimental import pallas as pl
from jax.experimental.pallas import tpu as pltpu
from jax.sharding import Mesh, PartitionSpec as P


BF = jnp.bfloat16
F32 = jnp.float32
CAP = 48
LANES = 128
NONE = 64.0


def kernel_call(fn, outs, limit_mib, *args, smem=0, scratch=()):
    vm = pl.BlockSpec(memory_space=pltpu.VMEM)
    sm = pl.BlockSpec(memory_space=pltpu.SMEM)
    return pl.pallas_call(
        fn,
        out_shape=outs,
        in_specs=[sm] * smem + [vm] * (len(args) - smem),
        out_specs=jax.tree.map(lambda _: vm, outs),
        scratch_shapes=list(scratch),
        compiler_params=pltpu.CompilerParams(vmem_limit_bytes=limit_mib << 20),
    )(*args)


def sds(shape, dtype=BF):
    return jax.ShapeDtypeStruct(shape, dtype)


def shift_z(a, k):
    n = lax.axis_size("z")
    return lax.ppermute(a, "z", [(i, (i + k) % n) for i in range(n)])


def shift(a, axis, k):
    n, cores = lax.axis_size(axis), lax.axis_size("c")
    pairs = []
    for c in range(cores):
        for i in range(n):
            j = (i + (k if c == 0 else -k)) % n
            pairs.append(
                (i * cores + c, j * cores + c) if axis == "x" else (c * n + i, c * n + j)
            )
    return lax.ppermute(a, ("x", "c") if axis == "x" else ("c", axis), pairs)


def swap_core(a):
    return lax.ppermute(a, "c", [(0, 1), (1, 0)])


def ring_gather(a, axis):
    behind = shift(a, axis, 1)
    ahead = shift(a, axis, -1)
    return behind, ahead, shift(behind, axis, 1)


def ring_scatter(own, behind, ahead, opp, axis):
    t = shift(opp, axis, 1)
    r = shift(behind, axis, -1)
    s = (ahead.astype(F32) + t.astype(F32)).astype(BF)
    q = shift(s, axis, 1)
    return own.astype(F32) + r.astype(F32) + q.astype(F32)


def prologue_kernel(tok, gain, router, svec, ids, out):
    x = tok[...].astype(F32)
    ms = jnp.mean(x * x, axis=-1, keepdims=True)
    normed = (x * lax.rsqrt(ms + 1e-06) * gain[...]).astype(BF)
    rows, width = normed.shape
    out[:, :width] = normed
    lane = lax.broadcasted_iota(jnp.int32, (rows, LANES), 1)
    expert = lane & 7
    row = lax.broadcasted_iota(jnp.int32, (rows, rows), 0)
    col = lax.broadcasted_iota(jnp.int32, (rows, rows), 1)
    eye = (row == col).astype(F32).astype(BF)
    ids_t = lax.dot_general(
        eye,
        ids[...].astype(F32).astype(BF),
        (((1,), (1,)), ((), ())),
        preferred_element_type=F32,
    )
    expert_f = expert.astype(F32)
    oh0 = (expert_f == ids_t[:, 0:1]).astype(F32)
    oh1 = (expert_f == ids_t[:, 1:2]).astype(F32)
    both = oh0 + oh1
    before = (col < row).astype(F32).astype(BF)
    count = jnp.dot(before, both.astype(BF), preferred_element_type=F32)
    slot = jnp.where(both > 0, count, NONE)
    logits = lax.dot_general(
        normed, router[...], (((1,), (1,)), ((), ())), preferred_element_type=F32
    )
    n_exp = logits.shape[1]
    l0 = jnp.sum(oh0[:, :n_exp] * logits, axis=-1, keepdims=True)
    l1 = jnp.sum(oh1[:, :n_exp] * logits, axis=-1, keepdims=True)
    w0 = jax.nn.sigmoid(l0 - l1)
    w = oh0 * w0 + oh1 * (1.0 - w0)
    gate = jax.nn.sigmoid(
        jnp.sum(normed.astype(F32) * svec[...], axis=-1, keepdims=True)
    )
    w_hi = w.astype(BF).astype(F32)
    g_hi = gate.astype(BF).astype(F32)
    ext = jnp.where(
        lane < 8,
        slot,
        jnp.where(
            lane < 16,
            w_hi,
            jnp.where(
                lane < 24,
                w - w_hi,
                jnp.where(lane == 24, g_hi, jnp.where(lane == 25, gate - g_hi, 0.0)),
            ),
        ),
    )
    out[:, width:] = ext.astype(BF)


def dispatch_kernel(me, *refs):
    out = refs[-1]
    width = out.shape[1]
    e = me[0]
    sel = (lax.broadcasted_iota(jnp.int32, (8, LANES), 1) == e).astype(F32).astype(BF)
    s_iota = lax.broadcasted_iota(jnp.int32, (CAP, LANES), 0).astype(F32)
    for j, block in enumerate(refs[:-1]):
        ext = block[:, width:]
        slot = lax.dot_general(sel, ext, (((1,), (1,)), ((), ())), preferred_element_type=F32)
        table = (s_iota == slot[0:1, :]).astype(F32).astype(BF)
        x = block[:, :width]
        out[j * CAP : (j + 1) * CAP, :] = jnp.dot(
            table, x, preferred_element_type=F32
        ).astype(BF)


def shared_kernel(*refs):
    toks, (sg, su, sd, out, xs) = refs[:-5], refs[-5:]
    width = out.shape[1]
    n = toks[0].shape[0]
    for j, block in enumerate(toks):
        xs[j * n : (j + 1) * n, :] = block[:, :width]
    step = 2 * n

    def one(i, _):
        at = pl.multiple_of(i * step, step)
        x = xs[pl.ds(at, step), :]
        g = jnp.dot(x, sg[...], preferred_element_type=F32)
        u = jnp.dot(x, su[...], preferred_element_type=F32)
        h = (jax.nn.silu(g) * u).astype(BF)
        out[pl.ds(at, step), :] = jnp.dot(
            h, sd[...], preferred_element_type=F32
        ).astype(BF)
        return 0

    lax.fori_loop(0, len(toks) // 2, one, 0)


def swiglu(y):
    return (jax.nn.silu(y[:, :LANES]) * y[:, LANES:]).astype(BF)


def times_transposed(x, w):
    return lax.dot_general(x, w, (((1,), (1,)), ((), ())), preferred_element_type=F32)


def early_kernel(n_shards, *refs):
    rows = refs[:4]
    wa = refs[4 : 4 + n_shards]
    wb = refs[4 + n_shards : 4 + 2 * n_shards]
    out, xs = refs[-2:]
    n, width = rows[0].shape
    half = width // 2
    for j, r in enumerate(rows):
        xs[j * n : (j + 1) * n, :] = r[...]

    def one(i, _):
        at = pl.multiple_of(i * n, n)
        x = xs[pl.ds(at, n), :]
        h = []
        for k in range(n_shards):
            gu = jnp.concatenate([wa[k][:width, :], wb[k][:width, :]], axis=1)
            h.append(swiglu(jnp.dot(x, gu, preferred_element_type=F32)))
        h = jnp.concatenate(h, axis=1)
        for d, w in enumerate((wa, wb)):
            down = jnp.concatenate([s[width:, :] for s in w], axis=1)
            out[pl.ds(at, n), d * half : (d + 1) * half] = times_transposed(h, down)
        return 0

    lax.fori_loop(0, 4, one, 0)


def late_kernel(rows0, rows1, rows2, rows3, la, lb, partial, own, behind, ahead, opp, hid):
    n, width = rows0.shape
    half = own.shape[1]
    gu = jnp.concatenate([la[:width, :], lb[:width, :]], axis=1)
    down = la[width:, :]
    outs = (own, behind, ahead, opp)
    for j, r in ((3, rows3), (1, rows1), (2, rows2), (0, rows0)):
        h = swiglu(jnp.dot(r[...], gu, preferred_element_type=F32))
        hid[j * n : (j + 1) * n, :] = h
        o = outs[j]
        o[...] = (
            partial[j * n : (j + 1) * n, :half] + times_transposed(h, down)
        ).astype(o.dtype)


def late_second_kernel(hid, lb, partial, own, behind, ahead, opp):
    n, half = own.shape
    down = lb[lb.shape[0] - half :, :]
    for j, o in enumerate((own, behind, ahead, opp)):
        o[...] = (
            partial[j * n : (j + 1) * n, half:]
            + times_transposed(hid[j * n : (j + 1) * n, :], down)
        ).astype(o.dtype)


def combine_kernel(lo, me, summed, shared, *refs):
    toks = refs[:8]
    mine, theirs = refs[8:]
    width = shared.shape[1]
    d = summed.shape[1]
    e = me[0]
    row = lax.broadcasted_iota(jnp.int32, (LANES, LANES), 0)
    pick_slot = (row == e).astype(F32).astype(BF)
    pick_w = ((row == e + 8) | (row == e + 16)).astype(F32).astype(BF)
    pick_g = ((row == 24) | (row == 25)).astype(F32).astype(BF)
    rows = summed[...].astype(BF)
    for j, block in enumerate(toks):
        ext = block[:, width:]
        n = ext.shape[0]
        slot = jnp.dot(ext, pick_slot, preferred_element_type=F32)
        w = jnp.dot(ext, pick_w, preferred_element_type=F32)[:, 0:1]
        g = jnp.dot(ext, pick_g, preferred_element_type=F32)[:, 0:1]
        lane = lax.broadcasted_iota(jnp.int32, (n, CAP), 1).astype(F32)
        table = (slot[:, :CAP] == lane).astype(F32).astype(BF)
        got = jnp.dot(
            table, rows[j * CAP : (j + 1) * CAP, :], preferred_element_type=F32
        )
        val = w * got + g * shared[j * n : (j + 1) * n, lo : lo + d].astype(F32)
        if j < 4:
            mine[j * n : (j + 1) * n, :] = val
        else:
            theirs[(j - 4) * n : (j - 3) * n, :] = val.astype(BF)


def body(
    tokens,
    norm_gain,
    router_weight,
    shared_gate_vector,
    expert_ids,
    gate_weight,
    up_weight,
    down_weight,
    shared_gate_weight,
    shared_up_weight,
    shared_down_weight,
):
    n_tok, width = tokens.shape
    half_d = width // 2
    me = (lax.axis_index("x") * 2 + lax.axis_index("c")).astype(jnp.int32)[None]

    wa = jnp.concatenate([gate_weight[0], down_weight[0, :half_d]], axis=0)
    wb = jnp.concatenate([up_weight[0], down_weight[0, half_d:]], axis=0)
    got_a, got_b = [wa], [wb]
    fa, ba, fb, bb = wa, wa, wb, wb
    for _ in range(3):
        fa, ba = shift_z(fa, 1), shift_z(ba, -1)
        fb, bb = shift_z(fb, 1), shift_z(bb, -1)
        got_a += [fa, ba]
        got_b += [fb, bb]
    last_a = shift_z(fa, 1)
    last_b = shift_z(bb, -1)

    ext = kernel_call(
        prologue_kernel,
        sds((n_tok, width + LANES)),
        16,
        tokens,
        norm_gain[None],
        router_weight.T,
        shared_gate_vector[None],
        expert_ids.T,
    )
    mine = [ext, *ring_gather(ext, "x")]
    toks = mine + [swap_core(t) for t in mine]
    rows = kernel_call(dispatch_kernel, sds((8 * CAP, width)), 16, me, *toks, smem=1)
    all_rows = [rows, *ring_gather(rows, "y")]
    shared = kernel_call(
        shared_kernel,
        sds((8 * n_tok, width)),
        24,
        *toks,
        shared_gate_weight,
        shared_up_weight,
        shared_down_weight,
        scratch=[pltpu.VMEM((8 * n_tok, width), BF)],
    )
    n = rows.shape[0]
    n_shards = len(got_a)
    partial = kernel_call(
        functools.partial(early_kernel, n_shards),
        sds((4 * n, width), F32),
        32,
        *all_rows,
        *got_a,
        *got_b,
        scratch=[pltpu.VMEM((4 * n, width), BF)],
    )
    pieces = (sds((n, half_d), F32), sds((n, half_d)), sds((n, half_d), F32), sds((n, half_d)))
    *first, hid = kernel_call(
        late_kernel, (*pieces, sds((4 * n, LANES))), 24, *all_rows, last_a, last_b, partial
    )
    second = kernel_call(late_second_kernel, pieces, 24, hid, last_b, partial)
    outs = []
    for d, parts in enumerate((first, second)):
        summed = ring_scatter(*parts, "y")
        mine_part, theirs = kernel_call(
            functools.partial(combine_kernel, d * half_d),
            (sds((4 * n_tok, half_d), F32), sds((4 * n_tok, half_d))),
            24,
            me,
            summed,
            shared,
            *toks,
            smem=1,
        )
        s = mine_part + swap_core(theirs).astype(F32)
        own, behind, ahead, opp = (s[i * n_tok : (i + 1) * n_tok] for i in range(4))
        outs.append(ring_scatter(own, behind.astype(BF), ahead, opp.astype(BF), "x"))
    return jnp.concatenate(outs, axis=1).astype(BF)


def solution(mesh):
    fine = Mesh(mesh.devices.reshape(4, 2, 4, 8), ("x", "c", "y", "z"))
    every = ("x", "c", "y", "z")

    return jax.shard_map(
        body,
        mesh=fine,
        in_specs=(
            P(every, None),
            P(),
            P(),
            P(),
            P(every, None),
            P(("x", "c"), None, ("y", "z")),
            P(("x", "c"), None, ("y", "z")),
            P(("x", "c"), None, ("y", "z")),
            P(None, ("x", "c")),
            P(None, ("x", "c")),
            P(("x", "c"), None),
        ),
        out_specs=P(every, None),
        check_vma=False,
    )
```

```python
import functools

import jax
import jax.numpy as jnp
from jax import lax
from jax.experimental import pallas as pl
from jax.experimental.pallas import tpu as pltpu
from jax.sharding import Mesh, PartitionSpec as P


BF = jnp.bfloat16
F32 = jnp.float32
CAP = 48
LANES = 128
NONE = 64.0

Y_PARTS = 2
X_PARTS = 2


def kernel_call(fn, outs, limit_mib, *args, smem=0, hbm=0, scratch=()):
    vm = pl.BlockSpec(memory_space=pltpu.VMEM)
    sm = pl.BlockSpec(memory_space=pltpu.SMEM)
    far = pl.BlockSpec(memory_space=pltpu.HBM)
    return pl.pallas_call(
        fn,
        out_shape=outs,
        in_specs=[sm] * smem + [vm] * (len(args) - smem - hbm) + [far] * hbm,
        out_specs=jax.tree.map(lambda _: vm, outs),
        scratch_shapes=list(scratch),
        compiler_params=pltpu.CompilerParams(vmem_limit_bytes=limit_mib << 20),
    )(*args)


def sds(shape, dtype=BF):
    return jax.ShapeDtypeStruct(shape, dtype)


def shift_z(a, k):
    n = lax.axis_size("z")
    return lax.ppermute(a, "z", [(i, (i + k) % n) for i in range(n)])


def shift(a, axis, k):
    n, cores = lax.axis_size(axis), lax.axis_size("c")
    pairs = []
    for c in range(cores):
        for i in range(n):
            j = (i + (k if c == 0 else -k)) % n
            pairs.append(
                (i * cores + c, j * cores + c) if axis == "x" else (c * n + i, c * n + j)
            )
    return lax.ppermute(a, ("x", "c") if axis == "x" else ("c", axis), pairs)


def swap_core(a):
    return lax.ppermute(a, "c", [(0, 1), (1, 0)])


def ring_gather(a, axis):
    behind = shift(a, axis, 1)
    ahead = shift(a, axis, -1)
    return behind, ahead, shift(behind, axis, 1)


def ring_scatter(own, behind, ahead, opp, axis):
    t = shift(opp, axis, 1)
    r = shift(behind, axis, -1)
    s = (ahead.astype(F32) + t.astype(F32)).astype(BF)
    q = shift(s, axis, 1)
    return own.astype(F32) + r.astype(F32) + q.astype(F32)


def prologue_kernel(
    tok_h, gain_h, router_h, svec_h, ids_h, gate_h, up_h, down_h,
    out, wa, wb, tok, gain, router, svec, ids, sems,
):
    width = gate_h.shape[1]
    half = width // 2
    small = [
        pltpu.make_async_copy(src, dst, sems.at[i])
        for i, (src, dst) in enumerate(
            ((tok_h, tok), (gain_h, gain), (router_h, router), (svec_h, svec), (ids_h, ids))
        )
    ]
    large = [
        pltpu.make_async_copy(src, dst, sems.at[5 + i])
        for i, (src, dst) in enumerate(
            (
                (gate_h.at[0], wa.at[pl.ds(0, width)]),
                (down_h.at[0, pl.ds(0, half)], wa.at[pl.ds(width, half)]),
                (up_h.at[0], wb.at[pl.ds(0, width)]),
                (down_h.at[0, pl.ds(half, half)], wb.at[pl.ds(width, half)]),
            )
        )
    ]
    for copy in small + large:
        copy.start()
    for copy in small:
        copy.wait()
    x = tok[...].astype(F32)
    ms = jnp.mean(x * x, axis=-1, keepdims=True)
    normed = (x * lax.rsqrt(ms + 1e-06) * gain[...]).astype(BF)
    rows = normed.shape[0]
    out[:, :width] = normed
    lane = lax.broadcasted_iota(jnp.int32, (rows, LANES), 1)
    expert = lane & 7
    row = lax.broadcasted_iota(jnp.int32, (rows, rows), 0)
    col = lax.broadcasted_iota(jnp.int32, (rows, rows), 1)
    eye = (row == col).astype(F32).astype(BF)
    ids_t = lax.dot_general(
        eye,
        ids[...].astype(F32).astype(BF),
        (((1,), (1,)), ((), ())),
        preferred_element_type=F32,
    )
    expert_f = expert.astype(F32)
    oh0 = (expert_f == ids_t[:, 0:1]).astype(F32)
    oh1 = (expert_f == ids_t[:, 1:2]).astype(F32)
    both = oh0 + oh1
    before = (col < row).astype(F32).astype(BF)
    count = jnp.dot(before, both.astype(BF), preferred_element_type=F32)
    slot = jnp.where(both > 0, count, NONE)
    logits = lax.dot_general(
        normed, router[...], (((1,), (1,)), ((), ())), preferred_element_type=F32
    )
    n_exp = logits.shape[1]
    l0 = jnp.sum(oh0[:, :n_exp] * logits, axis=-1, keepdims=True)
    l1 = jnp.sum(oh1[:, :n_exp] * logits, axis=-1, keepdims=True)
    w0 = jax.nn.sigmoid(l0 - l1)
    w = oh0 * w0 + oh1 * (1.0 - w0)
    gate = jax.nn.sigmoid(
        jnp.sum(normed.astype(F32) * svec[...], axis=-1, keepdims=True)
    )
    w_hi = w.astype(BF).astype(F32)
    g_hi = gate.astype(BF).astype(F32)
    ext = jnp.where(
        lane < 8,
        slot,
        jnp.where(
            lane < 16,
            w_hi,
            jnp.where(
                lane < 24,
                w - w_hi,
                jnp.where(lane == 24, g_hi, jnp.where(lane == 25, gate - g_hi, 0.0)),
            ),
        ),
    )
    out[:, width:] = ext.astype(BF)
    for copy in large:
        copy.wait()


def dispatch_kernel(me, own_tok, other_tok, out):
    width = out.shape[1]
    n = own_tok.shape[0] // 4
    e = me[0]
    sel = (lax.broadcasted_iota(jnp.int32, (8, LANES), 1) == e).astype(F32).astype(BF)
    s_iota = lax.broadcasted_iota(jnp.int32, (CAP, LANES), 0).astype(F32)

    def one(j, _):
        at = pl.ds(pl.multiple_of(j * n, n), n)
        for k, tok in enumerate((own_tok, other_tok)):
            slot = times_transposed(sel, tok[at, width:])
            table = (s_iota == slot[0:1, :]).astype(F32).astype(BF)
            to = pl.multiple_of((k * 4 + j) * CAP, CAP)
            out[pl.ds(to, CAP), :] = jnp.dot(
                table, tok[at, :width], preferred_element_type=F32
            ).astype(BF)
        return 0

    lax.fori_loop(0, 4, one, 0)


def shared_kernel(
    own_tok, other_tok, sg_h, su_h, sd_h, out, xs, sg, su, sd, sems
):
    copies = [
        pltpu.make_async_copy(src, dst, sems.at[i])
        for i, (src, dst) in enumerate(((sg_h, sg), (su_h, su), (sd_h, sd)))
    ]
    for copy in copies:
        copy.start()
    width = out.shape[1]
    n = own_tok.shape[0]
    for j, block in enumerate((own_tok, other_tok)):
        xs[j * n : (j + 1) * n, :] = block[:, :width]
    for copy in copies:
        copy.wait()
    step = n // 2

    def one(i, _):
        at = pl.multiple_of(i * step, step)
        x = xs[pl.ds(at, step), :]
        g = jnp.dot(x, sg[...], preferred_element_type=F32)
        u = jnp.dot(x, su[...], preferred_element_type=F32)
        h = (jax.nn.silu(g) * u).astype(BF)
        out[pl.ds(at, step), :] = jnp.dot(
            h, sd[...], preferred_element_type=F32
        ).astype(BF)
        return 0

    lax.fori_loop(0, 4, one, 0)


def swiglu(y):
    return (jax.nn.silu(y[:, :LANES]) * y[:, LANES:]).astype(BF)


def times_transposed(x, w):
    return lax.dot_general(x, w, (((1,), (1,)), ((), ())), preferred_element_type=F32)


def early_kernel(n_rows, n_shards, so_far, *refs):
    rows = refs[:n_rows]
    wa = refs[n_rows : n_rows + n_shards]
    wb = refs[n_rows + n_shards : n_rows + 2 * n_shards]
    rest = refs[n_rows + 2 * n_shards :]
    before, out, *xs = rest if so_far else (None, *rest)
    n, width = rows[0].shape
    half = width // 2

    def one(x, at):
        h = []
        for k in range(n_shards):
            gu = jnp.concatenate([wa[k][:width, :], wb[k][:width, :]], axis=1)
            h.append(swiglu(jnp.dot(x, gu, preferred_element_type=F32)))
        h = jnp.concatenate(h, axis=1)
        for d, w in enumerate((wa, wb)):
            down = jnp.concatenate([s[width:, :] for s in w], axis=1)
            y = times_transposed(h, down)
            cols = slice(d * half, (d + 1) * half)
            if so_far:
                y = y + before[pl.ds(at, n), cols]
            out[pl.ds(at, n), cols] = y

    if n_rows == 1:
        one(rows[0][...], 0)
        return
    (xs,) = xs
    for j, r in enumerate(rows):
        xs[j * n : (j + 1) * n, :] = r[...]

    def step(i, _):
        at = pl.multiple_of(i * n, n)
        one(xs[pl.ds(at, n), :], at)
        return 0

    lax.fori_loop(0, n_rows, step, 0)


def late_kernel(whole, rows0, rows1, rows2, rows3, la, lb, part, part_opp, own, behind, ahead, opp, *hid):
    n, width = rows0.shape
    size = own.shape[1]
    gu = jnp.concatenate([la[:width, :], lb[:width, :]], axis=1)
    down = la[width:, :]
    if whole:
        down = jnp.concatenate([down, lb[width:, :]], axis=0)
    for j, r, o in ((3, rows3, opp), (1, rows1, behind), (2, rows2, ahead), (0, rows0, own)):
        h = swiglu(jnp.dot(r[...], gu, preferred_element_type=F32))
        if not whole:
            hid[0][j * n : (j + 1) * n, :] = h
        so_far = part_opp[:, :size] if j == 3 else part[j * n : (j + 1) * n, :size]
        o[...] = (so_far + times_transposed(h, down)).astype(o.dtype)


def late_second_kernel(hid, lb, part, part_opp, own, behind, ahead, opp):
    n, half = own.shape
    down = lb[lb.shape[0] - half :, :]
    for j, o in enumerate((own, behind, ahead, opp)):
        so_far = part_opp[:, half:] if j == 3 else part[j * n : (j + 1) * n, half:]
        o[...] = (so_far + times_transposed(hid[j * n : (j + 1) * n, :], down)).astype(o.dtype)


def combine_kernel(lo, me, shared, own_tok, other_tok, *refs):
    *summed, mine, theirs, rows = refs
    width = shared.shape[1]
    d = mine.shape[1]
    n = own_tok.shape[0] // 4
    e = me[0]
    row = lax.broadcasted_iota(jnp.int32, (LANES, LANES), 0)
    pick_slot = (row == e).astype(F32).astype(BF)
    pick_w = ((row == e + 8) | (row == e + 16)).astype(F32).astype(BF)
    pick_g = ((row == 24) | (row == 25)).astype(F32).astype(BF)
    lane = lax.broadcasted_iota(jnp.int32, (n, CAP), 1).astype(F32)
    for i, r in enumerate(summed):
        rows[:, i * r.shape[1] : (i + 1) * r.shape[1]] = r[...].astype(BF)

    def one(j, _):
        at = pl.ds(pl.multiple_of(j * n, n), n)
        for k, (tok, out) in enumerate(((own_tok, mine), (other_tok, theirs))):
            ext = tok[at, width:]
            slot = jnp.dot(ext, pick_slot, preferred_element_type=F32)
            w = jnp.dot(ext, pick_w, preferred_element_type=F32)[:, 0:1]
            g = jnp.dot(ext, pick_g, preferred_element_type=F32)[:, 0:1]
            table = (slot[:, :CAP] == lane).astype(F32).astype(BF)
            of = pl.multiple_of((k * 4 + j) * CAP, CAP)
            got = jnp.dot(table, rows[pl.ds(of, CAP), :], preferred_element_type=F32)
            there = pl.ds(pl.multiple_of((k * 4 + j) * n, n), n)
            val = w * got + g * shared[there, lo : lo + d].astype(F32)
            out[at, :] = val.astype(out.dtype)
        return 0

    lax.fori_loop(0, 4, one, 0)


def body(
    tokens,
    norm_gain,
    router_weight,
    shared_gate_vector,
    expert_ids,
    gate_weight,
    up_weight,
    down_weight,
    shared_gate_weight,
    shared_up_weight,
    shared_down_weight,
):
    n_tok, width = tokens.shape
    half_d = width // 2
    me = (lax.axis_index("x") * 2 + lax.axis_index("c")).astype(jnp.int32)[None]

    small = (
        tokens,
        norm_gain[None],
        router_weight.T,
        shared_gate_vector[None],
        expert_ids.T,
    )
    stream = sds((width + half_d, LANES))
    ext, wa, wb = kernel_call(
        prologue_kernel,
        (sds((n_tok, width + LANES)), stream, stream),
        60,
        *small,
        gate_weight,
        up_weight,
        down_weight,
        hbm=8,
        scratch=[pltpu.VMEM(a.shape, a.dtype) for a in small]
        + [pltpu.SemaphoreType.DMA((9,))],
    )

    mine = jnp.concatenate([ext, *ring_gather(ext, "x")], axis=0)
    toks = (mine, swap_core(mine))

    got_a, got_b = [wa], [wb]
    fa, ba, fb, bb = wa, wa, wb, wb
    for _ in range(3):
        fa, ba = shift_z(fa, 1), shift_z(ba, -1)
        fb, bb = shift_z(fb, 1), shift_z(bb, -1)
        got_a += [fa, ba]
        got_b += [fb, bb]
    last_a = shift_z(fa, 1)
    last_b = shift_z(bb, -1)

    rows = kernel_call(dispatch_kernel, sds((8 * CAP, width)), 16, me, *toks, smem=1)
    all_rows = [rows, *ring_gather(rows, "y")]
    shared = kernel_call(
        shared_kernel,
        sds((8 * n_tok, width)),
        24,
        *toks,
        shared_gate_weight,
        shared_up_weight,
        shared_down_weight,
        hbm=3,
        scratch=[pltpu.VMEM((8 * n_tok, width), BF)]
        + [
            pltpu.VMEM(a.shape, a.dtype)
            for a in (shared_gate_weight, shared_up_weight, shared_down_weight)
        ]
        + [pltpu.SemaphoreType.DMA((3,))],
    )
    n = rows.shape[0]
    n_shards = len(got_a)

    def early(rows, lo, hi, *before):
        m = len(rows)
        return kernel_call(
            functools.partial(early_kernel, m, hi - lo, len(before)),
            sds((m * n, width), F32),
            32,
            *rows,
            *got_a[lo:hi],
            *got_b[lo:hi],
            *before,
            scratch=[pltpu.VMEM((m * n, width), BF)] if m > 1 else [],
        )

    part = early(all_rows[:3], 0, n_shards - 2)
    part = early(all_rows[:3], n_shards - 2, n_shards, part)
    part_opp = early(all_rows[3:], 0, n_shards)

    def pieces(d):
        return (sds((n, d), F32), sds((n, d)), sds((n, d), F32), sds((n, d)))

    late = (*all_rows, last_a, last_b, part, part_opp)
    if Y_PARTS == 1:
        all_parts = [kernel_call(functools.partial(late_kernel, True), pieces(width), 24, *late)]
    else:
        *first, hid = kernel_call(
            functools.partial(late_kernel, False), (*pieces(half_d), sds((4 * n, LANES))), 24, *late
        )
        second = kernel_call(late_second_kernel, pieces(half_d), 24, hid, last_b, part, part_opp)
        all_parts = [first, second]
    summed = [ring_scatter(*parts, "y") for parts in all_parts]

    def give_back(lo, d, halves):
        mine_part, theirs = kernel_call(
            functools.partial(combine_kernel, lo),
            (sds((4 * n_tok, d), F32), sds((4 * n_tok, d))),
            24,
            me,
            shared,
            *toks,
            *halves,
            smem=1,
            scratch=[pltpu.VMEM((n, d), BF)],
        )
        s = mine_part + swap_core(theirs).astype(F32)
        own, behind, ahead, opp = (s[i * n_tok : (i + 1) * n_tok] for i in range(4))
        return ring_scatter(own, behind.astype(BF), ahead, opp.astype(BF), "x")

    if X_PARTS == 1:
        return give_back(0, width, summed).astype(BF)
    outs = [give_back(i * half_d, half_d, [h]) for i, h in enumerate(summed)]
    return jnp.concatenate(outs, axis=1).astype(BF)


def solution(mesh):
    fine = Mesh(mesh.devices.reshape(4, 2, 4, 8), ("x", "c", "y", "z"))
    every = ("x", "c", "y", "z")

    return jax.shard_map(
        body,
        mesh=fine,
        in_specs=(
            P(every, None),
            P(),
            P(),
            P(),
            P(every, None),
            P(("x", "c"), None, ("y", "z")),
            P(("x", "c"), None, ("y", "z")),
            P(("x", "c"), None, ("y", "z")),
            P(None, ("x", "c")),
            P(None, ("x", "c")),
            P(("x", "c"), None),
        ),
        out_specs=P(every, None),
        check_vma=False,
    )
```

```python
import functools

import jax
import jax.numpy as jnp
from jax import lax
from jax.experimental import pallas as pl
from jax.experimental.pallas import tpu as pltpu
from jax.sharding import Mesh, PartitionSpec as P


BF = jnp.bfloat16
F32 = jnp.float32
CAP = 48
LANES = 128
NONE = 64.0


def kernel_call(fn, outs, limit_mib, *args, smem=0, hbm=0, scratch=()):
    vm = pl.BlockSpec(memory_space=pltpu.VMEM)
    sm = pl.BlockSpec(memory_space=pltpu.SMEM)
    far = pl.BlockSpec(memory_space=pltpu.HBM)
    return pl.pallas_call(
        fn,
        out_shape=outs,
        in_specs=[sm] * smem + [vm] * (len(args) - smem - hbm) + [far] * hbm,
        out_specs=jax.tree.map(lambda _: vm, outs),
        scratch_shapes=list(scratch),
        compiler_params=pltpu.CompilerParams(vmem_limit_bytes=limit_mib << 20),
    )(*args)


def sds(shape, dtype=BF):
    return jax.ShapeDtypeStruct(shape, dtype)


def shift_z(a, k):
    n = lax.axis_size("z")
    return lax.ppermute(a, "z", [(i, (i + k) % n) for i in range(n)])


def shift(a, axis, k):
    n, cores = lax.axis_size(axis), lax.axis_size("c")
    pairs = []
    for c in range(cores):
        for i in range(n):
            j = (i + (k if c == 0 else -k)) % n
            pairs.append(
                (i * cores + c, j * cores + c) if axis == "x" else (c * n + i, c * n + j)
            )
    return lax.ppermute(a, ("x", "c") if axis == "x" else ("c", axis), pairs)


def swap_core(a):
    return lax.ppermute(a, "c", [(0, 1), (1, 0)])


def ring_gather(a, axis):
    behind = shift(a, axis, 1)
    ahead = shift(a, axis, -1)
    return behind, ahead, shift(behind, axis, 1)


def ring_scatter(own, behind, ahead, opp, axis):
    t = shift(opp, axis, 1)
    r = shift(behind, axis, -1)
    s = (ahead.astype(F32) + t.astype(F32)).astype(BF)
    q = shift(s, axis, 1)
    return own.astype(F32) + r.astype(F32) + q.astype(F32)


def prologue_kernel(
    tok_h, gain_h, router_h, svec_h, ids_h, gate_h, up_h, down_h,
    out, wa, wb, tok, gain, router, svec, ids, sems,
):
    width = gate_h.shape[1]
    half = width // 2
    small = [
        pltpu.make_async_copy(src, dst, sems.at[i])
        for i, (src, dst) in enumerate(
            ((tok_h, tok), (gain_h, gain), (router_h, router), (svec_h, svec), (ids_h, ids))
        )
    ]
    large = [
        pltpu.make_async_copy(src, dst, sems.at[5 + i])
        for i, (src, dst) in enumerate(
            (
                (gate_h.at[0], wa.at[pl.ds(0, width)]),
                (down_h.at[0, pl.ds(0, half)], wa.at[pl.ds(width, half)]),
                (up_h.at[0], wb.at[pl.ds(0, width)]),
                (down_h.at[0, pl.ds(half, half)], wb.at[pl.ds(width, half)]),
            )
        )
    ]
    for copy in small + large:
        copy.start()
    for copy in small:
        copy.wait()
    x = tok[...].astype(F32)
    ms = jnp.mean(x * x, axis=-1, keepdims=True)
    normed = (x * lax.rsqrt(ms + 1e-06) * gain[...]).astype(BF)
    rows = normed.shape[0]
    out[:, :width] = normed
    lane = lax.broadcasted_iota(jnp.int32, (rows, LANES), 1)
    expert = lane & 7
    row = lax.broadcasted_iota(jnp.int32, (rows, rows), 0)
    col = lax.broadcasted_iota(jnp.int32, (rows, rows), 1)
    eye = (row == col).astype(F32).astype(BF)
    ids_t = lax.dot_general(
        eye,
        ids[...].astype(F32).astype(BF),
        (((1,), (1,)), ((), ())),
        preferred_element_type=F32,
    )
    expert_f = expert.astype(F32)
    oh0 = (expert_f == ids_t[:, 0:1]).astype(F32)
    oh1 = (expert_f == ids_t[:, 1:2]).astype(F32)
    both = oh0 + oh1
    before = (col < row).astype(F32).astype(BF)
    count = jnp.dot(before, both.astype(BF), preferred_element_type=F32)
    slot = jnp.where(both > 0, count, NONE)
    logits = lax.dot_general(
        normed, router[...], (((1,), (1,)), ((), ())), preferred_element_type=F32
    )
    n_exp = logits.shape[1]
    l0 = jnp.sum(oh0[:, :n_exp] * logits, axis=-1, keepdims=True)
    l1 = jnp.sum(oh1[:, :n_exp] * logits, axis=-1, keepdims=True)
    w0 = jax.nn.sigmoid(l0 - l1)
    w = oh0 * w0 + oh1 * (1.0 - w0)
    gate = jax.nn.sigmoid(
        jnp.sum(normed.astype(F32) * svec[...], axis=-1, keepdims=True)
    )
    w_hi = w.astype(BF).astype(F32)
    g_hi = gate.astype(BF).astype(F32)
    ext = jnp.where(
        lane < 8,
        slot,
        jnp.where(
            lane < 16,
            w_hi,
            jnp.where(
                lane < 24,
                w - w_hi,
                jnp.where(lane == 24, g_hi, jnp.where(lane == 25, gate - g_hi, 0.0)),
            ),
        ),
    )
    out[:, width:] = ext.astype(BF)
    for copy in large:
        copy.wait()


def dispatch_kernel(me, own_tok, other_tok, out):
    width = out.shape[1]
    n = own_tok.shape[0] // 4
    e = me[0]
    x, c = e // 2, e % 2
    sel = (lax.broadcasted_iota(jnp.int32, (8, LANES), 1) == e).astype(F32).astype(BF)
    s_iota = lax.broadcasted_iota(jnp.int32, (CAP, LANES), 0).astype(F32)

    def one(j, _):
        at = pl.ds(pl.multiple_of(j * n, n), n)
        up = jnp.where(j == 0, 0, jnp.where(j == 1, 3, jnp.where(j == 2, 1, 2)))
        for tok, core in ((own_tok, c), (other_tok, 1 - c)):
            slot = times_transposed(sel, tok[at, width:])
            table = (s_iota == slot[0:1, :]).astype(F32).astype(BF)
            chip = (x + jnp.where(core == 0, up, 4 - up)) % 4
            to = pl.multiple_of((chip * 2 + core) * CAP, CAP)
            out[pl.ds(to, CAP), :] = jnp.dot(
                table, tok[at, :width], preferred_element_type=F32
            ).astype(BF)
        return 0

    lax.fori_loop(0, 4, one, 0)


def shared_kernel(
    own_tok, other_tok, sg_h, su_h, sd_h, mine, theirs, sg, su, sd, sems
):
    copies = [
        pltpu.make_async_copy(src, dst, sems.at[i])
        for i, (src, dst) in enumerate(((sg_h, sg), (su_h, su), (sd_h, sd)))
    ]
    for copy in copies:
        copy.start()
    width = mine.shape[1]
    step = own_tok.shape[0] // 2
    for copy in copies:
        copy.wait()

    def one(i, _):
        at = pl.ds(pl.multiple_of(i * step, step), step)
        for tok, out in ((own_tok, mine), (other_tok, theirs)):
            x = tok[at, :width]
            g = jnp.dot(x, sg[...], preferred_element_type=F32)
            u = jnp.dot(x, su[...], preferred_element_type=F32)
            h = (jax.nn.silu(g) * u).astype(BF)
            out[at, :] = jnp.dot(h, sd[...], preferred_element_type=F32).astype(BF)
        return 0

    lax.fori_loop(0, 2, one, 0)


def swiglu(y):
    return (jax.nn.silu(y[:, :LANES]) * y[:, LANES:]).astype(BF)


def times_transposed(x, w):
    return lax.dot_general(x, w, (((1,), (1,)), ((), ())), preferred_element_type=F32)


def early_kernel(n_rows, n_shards, so_far, *refs):
    rows = refs[:n_rows]
    wa = refs[n_rows : n_rows + n_shards]
    wb = refs[n_rows + n_shards : n_rows + 2 * n_shards]
    rest = refs[n_rows + 2 * n_shards :]
    before, out, *xs = rest if so_far else (None, *rest)
    n, width = rows[0].shape
    half = width // 2

    def one(x, at):
        n = x.shape[0]
        h = []
        for k in range(n_shards):
            gu = jnp.concatenate([wa[k][:width, :], wb[k][:width, :]], axis=1)
            h.append(swiglu(jnp.dot(x, gu, preferred_element_type=F32)))
        h = jnp.concatenate(h, axis=1)
        for d, w in enumerate((wa, wb)):
            down = jnp.concatenate([s[width:, :] for s in w], axis=1)
            y = times_transposed(h, down)
            cols = slice(d * half, (d + 1) * half)
            if so_far:
                y = y + before[pl.ds(at, n), cols]
            out[pl.ds(at, n), cols] = y

    if n_rows == 1:
        one(rows[0][...], 0)
        return
    (xs,) = xs
    for j, r in enumerate(rows):
        xs[j * n : (j + 1) * n, :] = r[...]

    size = n_rows * n // 2

    def step(i, _):
        at = pl.multiple_of(i * size, size)
        one(xs[pl.ds(at, size), :], at)
        return 0

    lax.fori_loop(0, 2, step, 0)


def late_kernel(
    rows0, rows1, rows2, rows3, la, lb, part, part_opp, own, behind, ahead, opp, hid
):
    n, width = rows0.shape
    size = own.shape[1]
    gu = jnp.concatenate([la[:width, :], lb[:width, :]], axis=1)
    down = la[width:, :]
    for j, r, o in ((3, rows3, opp), (1, rows1, behind), (2, rows2, ahead), (0, rows0, own)):
        h = swiglu(jnp.dot(r[...], gu, preferred_element_type=F32))
        hid[j * n : (j + 1) * n, :] = h
        so_far = part_opp[:, :size] if j == 3 else part[j * n : (j + 1) * n, :size]
        o[...] = (so_far + times_transposed(h, down)).astype(o.dtype)


def late_second_kernel(hid, lb, part, part_opp, own, behind, ahead, opp):
    n, half = own.shape
    down = lb[lb.shape[0] - half :, :]
    for j, o in enumerate((own, behind, ahead, opp)):
        so_far = part_opp[:, half:] if j == 3 else part[j * n : (j + 1) * n, half:]
        o[...] = (so_far + times_transposed(hid[j * n : (j + 1) * n, :], down)).astype(o.dtype)


def final_kernel(ext, shared, *refs):
    *halves, out = refs
    n = ext.shape[0]
    tail = ext[:, out.shape[1] :].astype(F32)
    gate = tail[:, 24:25] + tail[:, 25:26]
    lane = lax.broadcasted_iota(jnp.int32, (n, CAP), 1).astype(F32)
    experts = halves[0].shape[0] // CAP
    d = halves[0].shape[1]
    for i, rows in enumerate(halves):
        cols = slice(i * d, (i + 1) * d)
        val = gate * shared[:, cols]
        for e in range(experts):
            table = (tail[:, e : e + 1] == lane).astype(F32).astype(BF)
            got = jnp.dot(
                table, rows[e * CAP : (e + 1) * CAP, :], preferred_element_type=F32
            )
            val = val + (tail[:, 8 + e : 9 + e] + tail[:, 16 + e : 17 + e]) * got
        out[:, cols] = val.astype(BF)


def body(
    tokens,
    norm_gain,
    router_weight,
    shared_gate_vector,
    expert_ids,
    gate_weight,
    up_weight,
    down_weight,
    shared_gate_weight,
    shared_up_weight,
    shared_down_weight,
):
    n_tok, width = tokens.shape
    half_d = width // 2
    me = (lax.axis_index("x") * 2 + lax.axis_index("c")).astype(jnp.int32)[None]

    small = (
        tokens,
        norm_gain[None],
        router_weight.T,
        shared_gate_vector[None],
        expert_ids.T,
    )
    stream = sds((width + half_d, LANES))
    ext, wa, wb = kernel_call(
        prologue_kernel,
        (sds((n_tok, width + LANES)), stream, stream),
        60,
        *small,
        gate_weight,
        up_weight,
        down_weight,
        hbm=8,
        scratch=[pltpu.VMEM(a.shape, a.dtype) for a in small]
        + [pltpu.SemaphoreType.DMA((9,))],
    )

    mine = jnp.concatenate([ext, *ring_gather(ext, "x")], axis=0)
    toks = (mine, swap_core(mine))

    got_a, got_b = [wa], [wb]
    fa, ba, fb, bb = wa, wa, wb, wb
    for _ in range(3):
        fa, ba = shift_z(fa, 1), shift_z(ba, -1)
        fb, bb = shift_z(fb, 1), shift_z(bb, -1)
        got_a += [fa, ba]
        got_b += [fb, bb]
    last_a = shift_z(fa, 1)
    last_b = shift_z(bb, -1)

    rows = kernel_call(dispatch_kernel, sds((8 * CAP, width)), 16, me, *toks, smem=1)
    all_rows = [rows, *ring_gather(rows, "y")]
    mine_part, theirs = kernel_call(
        shared_kernel,
        (sds((4 * n_tok, width)), sds((4 * n_tok, width))),
        12,
        *toks,
        shared_gate_weight,
        shared_up_weight,
        shared_down_weight,
        hbm=3,
        scratch=[
            pltpu.VMEM(a.shape, a.dtype)
            for a in (shared_gate_weight, shared_up_weight, shared_down_weight)
        ]
        + [pltpu.SemaphoreType.DMA((3,))],
    )
    s = mine_part.astype(F32) + swap_core(theirs).astype(F32)
    own, behind, ahead, opp = (s[i * n_tok : (i + 1) * n_tok] for i in range(4))
    shared = ring_scatter(own, behind.astype(BF), ahead, opp.astype(BF), "x")

    n = rows.shape[0]
    n_shards = len(got_a)

    def early(rows, lo, hi, *before):
        m = len(rows)
        return kernel_call(
            functools.partial(early_kernel, m, hi - lo, len(before)),
            sds((m * n, width), F32),
            12,
            *rows,
            *got_a[lo:hi],
            *got_b[lo:hi],
            *before,
            scratch=[pltpu.VMEM((m * n, width), BF)] if m > 1 else [],
        )

    part = early(all_rows[:3], 0, 4)
    part = early(all_rows[:3], 4, n_shards, part)
    part_opp = early(all_rows[3:], 0, n_shards)

    def pieces(d):
        return (sds((n, d), F32), sds((n, d)), sds((n, d), F32), sds((n, d)))

    *first, hid = kernel_call(
        late_kernel,
        (*pieces(half_d), sds((4 * n, LANES))),
        12,
        *all_rows,
        last_a,
        last_b,
        part,
        part_opp,
    )
    second = kernel_call(late_second_kernel, pieces(half_d), 12, hid, last_b, part, part_opp)
    summed = [ring_scatter(*parts, "y").astype(BF) for parts in (first, second)]
    back = lax.all_to_all(
        jnp.concatenate(summed, axis=1), ("x", "c"), 0, 0, tiled=True
    )
    return kernel_call(final_kernel, sds((n_tok, width)), 16, ext, shared, back)


def solution(mesh):
    fine = Mesh(mesh.devices.reshape(4, 2, 4, 8), ("x", "c", "y", "z"))
    every = ("x", "c", "y", "z")

    return jax.shard_map(
        body,
        mesh=fine,
        in_specs=(
            P(every, None),
            P(),
            P(),
            P(),
            P(every, None),
            P(("x", "c"), None, ("y", "z")),
            P(("x", "c"), None, ("y", "z")),
            P(("x", "c"), None, ("y", "z")),
            P(None, ("x", "c")),
            P(None, ("x", "c")),
            P(("x", "c"), None),
        ),
        out_specs=P(every, None),
        check_vma=False,
    )
```
